32 devices in a mesh: seg: 32 (over z, y, x, core).
Axes of the slice: x: 2, y: 2, z: 4, core: 2. Of those that a mesh axis runs over, the one named last changes fastest.
Arguments:
- cam_jac: bfloat16 [18, 512, 512], P(None, 'seg'), may hold values from -0.25 to 0.25
- point_jac: bfloat16 [6, 512, 512], P(None, 'seg'), may hold values from -6 to 6
- obs_point: int32 [512, 512], P('seg'), may hold values from 0 to 1791, as said below
- obs_count: int32 [512], P('seg'), may hold values from 64 to 512, as said below
- back_list: int32 [32, 384], P('seg'), may hold values from 0 to 1023, as said below
- front_list: int32 [32, 384], P('seg'), may hold values from 0 to 1023, as said below
- point_damp: float32 [32768], P('seg'), may hold values from 0.5 to 4
- cam_damp: float32 [512], P('seg'), may hold values from 0.1 to 1
- right_side: float32 [9, 512], P(None, 'seg'), may hold values from -25 to 25
- start_guess: float32 [9, 512], P(None, 'seg'), may hold values from -3 to 3
Outputs:
- camera_step: float32 [9, 512], P(None, 'seg')
- residual: float32 [9, 512], P(None, 'seg')
The draws below stay inside these ranges and needn't reach their ends.
Inputs may be any that keep to these rules, and one draw needn't show every extreme that they name: `obs_point`: entries below 1024 name the segment's own points; an entry e from 1024 to 1407 names entry e - 1024 of the previous segment's back_list, and a larger one entry e - 1408 of the next segment's front_list. Keyframes of the first segment name no back slot, those of the last segment no front slot. `obs_count`: slots at or past a keyframe's count are padding. Every segment has a keyframe whose slots are all used. `back_list`: each row holds 384 distinct own points of the segment; no point stands on both lists of its segment. `front_list`: each row holds 384 distinct own points of the segment; no point stands on both lists of its segment.
All inputs are finite; a program needn't handle non-finite values.
Results may differ from the reference program's by a relative error of at most 0.0005.
Values sent between devices are 32-bit elements; how exact they have to be, the bound alone decides.
A program may use at most 64 MiB of HBM per device.

```python
import math
import jax
import jax.numpy as jnp
from jax import lax

CAM_DEV = 16
OBS_CAM = 512
P_DEV = 1024
ITERS = 2
BORDER = 384
SEGMENTS = 32
CAMERAS = 512
POINTS = 32768


def border_lists(key):
    seg_keys = jax.random.split(jax.random.fold_in(key, 11), SEGMENTS)
    orders = jax.vmap(lambda seg_key: jax.random.permutation(seg_key, P_DEV))(seg_keys)
    return (orders[:, :BORDER].astype(jnp.int32), orders[:, BORDER:2 * BORDER].astype(jnp.int32))


def draw_back_list(key, part):
    return border_lists(key)[0]


def draw_front_list(key, part):
    return border_lists(key)[1]


def draw_obs_point(key, part):
    side_key, own_key, slot_key = jax.random.split(jax.random.fold_in(key, 3), 3)
    side_pick = jax.random.randint(side_key, (CAMERAS, OBS_CAM), 0, 4)
    segment = (jnp.arange(CAMERAS, dtype=jnp.int32) // CAM_DEV)[:, None]
    own_pick = jax.random.randint(own_key, (CAMERAS, OBS_CAM), 0, P_DEV)
    slot_pick = jax.random.randint(slot_key, (CAMERAS, OBS_CAM), 0, BORDER)
    back_side = (side_pick == 0) & (segment > 0)
    front_side = (side_pick == 1) & (segment < SEGMENTS - 1)
    result = jnp.where(back_side, P_DEV + slot_pick, jnp.where(front_side, P_DEV + BORDER + slot_pick, own_pick))
    return result.astype(jnp.int32)


def draw_obs_count(key, part):
    high_key, count_key, full_key = jax.random.split(jax.random.fold_in(key, 5), 3)
    high_cap = jax.random.randint(high_key, (SEGMENTS,), OBS_CAM // 2, OBS_CAM + 1)
    high_rows = jnp.repeat(high_cap, CAM_DEV)
    low_rows = high_rows // 4
    counts = jax.random.randint(count_key, (CAMERAS,), low_rows, high_rows + 1)
    full_pos = jnp.repeat(jax.random.randint(full_key, (SEGMENTS,), 0, CAM_DEV), CAM_DEV)
    marked = jnp.arange(CAMERAS, dtype=jnp.int32) % CAM_DEV == full_pos
    return jnp.where(marked, OBS_CAM, counts).astype(jnp.int32)


def draw_right_side(key, part):
    first_key = jax.random.fold_in(jax.random.fold_in(key, 9), 0)
    position = jnp.arange(CAMERAS, dtype=jnp.float32) / CAMERAS
    random_part = jnp.clip(jax.random.normal(first_key, (9, CAMERAS), jnp.float32), -6.0, 6.0)
    rising = 3.0 ** position
    return (random_part * rising[None, :]).astype(jnp.float32)


def steps_of(key, extent, pieces, low, top_value):
    def one(dim, shards_of):
        steps = jax.random.uniform(jax.random.fold_in(jax.random.fold_in(key, 6), dim), (shards_of,), jnp.float32, low / len(pieces), top_value / len(pieces))
        return jnp.repeat(jnp.exp(steps), extent[dim] // shards_of).reshape((-1,) + (1,) * (len(extent) - dim - 1))

    gain = one(*pieces[0])
    for cut in pieces[1:]:
        gain = gain * one(*cut)
    return gain


def scatter_about(rng, shape, width, most, pieces=(), kind=jnp.bfloat16):
    values = width * jax.random.normal(rng, shape, jnp.float32)
    if pieces:
        values = values * steps_of(rng, shape, pieces, -0.22, 0.18)
    return jnp.clip(values, -most, most).astype(kind)


def setup_inputs(seed: int = 0) -> dict:
    arg_keys = jax.random.split(jax.random.key(seed), 11)
    cam_jac = scatter_about(arg_keys[0], (18, CAMERAS, OBS_CAM), OBS_CAM ** -0.5, 0.25, ((1, 32),))
    point_jac = scatter_about(arg_keys[1], (6, CAMERAS, OBS_CAM), 1.0, 6.0, ((1, 32),))
    obs_point = draw_obs_point(jax.random.fold_in(arg_keys[10], 71), 0)
    obs_count = draw_obs_count(jax.random.fold_in(arg_keys[10], 71), 0)
    back_list = draw_back_list(jax.random.fold_in(arg_keys[10], 71), 0)
    front_list = draw_front_list(jax.random.fold_in(arg_keys[10], 71), 0)
    point_damp = jnp.clip(jnp.exp(math.log(4.0) - 2.0794415 * jax.random.uniform(arg_keys[6], (POINTS,), jnp.float32) ** steps_of(arg_keys[6], (POINTS,), ((0, 32),), -0.2, 0.2)), 0.5, 4.0)
    cam_damp = jnp.clip(jnp.exp(math.log(1.0) - 2.3025851 * jax.random.uniform(arg_keys[7], (CAMERAS,), jnp.float32) ** steps_of(arg_keys[7], (CAMERAS,), ((0, 32),), -0.2, 0.2)), 0.1, 1.0)
    right_side = draw_right_side(jax.random.fold_in(arg_keys[10], 71), 0)
    start_guess = scatter_about(arg_keys[9], (9, CAMERAS), 0.5, 3.0, ((1, 32),), jnp.float32)
    return {"cam_jac": cam_jac, "point_jac": point_jac, "obs_point": obs_point, "obs_count": obs_count, "back_list": back_list, "front_list": front_list, "point_damp": point_damp, "cam_damp": cam_damp, "right_side": right_side, "start_guess": start_guess}


ENTRY_PAIRS = ((0, 0), (0, 1), (0, 2), (1, 1), (1, 2), (2, 2))


def slot_weights(obs_count, slot_total):
    positions = lax.broadcasted_iota(jnp.int32, (obs_count.shape[0], slot_total), 1)
    return (positions < obs_count[:, None]).astype(jnp.float32)


def global_points(obs_point, back_list, front_list):
    segment = (jnp.arange(obs_point.shape[0], dtype=jnp.int32) // CAM_DEV)[:, None]
    prev_seg = jnp.clip(segment - 1, 0, SEGMENTS - 1)
    next_seg = jnp.clip(segment + 1, 0, SEGMENTS - 1)
    back_slot = jnp.clip(obs_point - P_DEV, 0, BORDER - 1)
    front_slot = jnp.clip(obs_point - P_DEV - BORDER, 0, BORDER - 1)
    own_global = segment * P_DEV + obs_point
    from_back = prev_seg * P_DEV + back_list[prev_seg, back_slot]
    from_front = next_seg * P_DEV + front_list[next_seg, front_slot]
    result = jnp.where(obs_point < P_DEV, own_global, jnp.where(obs_point < P_DEV + BORDER, from_back, from_front))
    return result.astype(jnp.int32).reshape(-1)


def symmetric_inverse(entries):
    cofactors = [entries[3] * entries[5] - entries[4] * entries[4],
                 entries[2] * entries[4] - entries[1] * entries[5],
                 entries[1] * entries[4] - entries[2] * entries[3],
                 entries[0] * entries[5] - entries[2] * entries[2],
                 entries[1] * entries[2] - entries[0] * entries[4],
                 entries[0] * entries[3] - entries[1] * entries[1]]
    determinant = entries[0] * cofactors[0] + entries[1] * cofactors[1] + entries[2] * cofactors[2]
    return [member / determinant for member in cofactors]


def apply_inverse(inverse, point_sums):
    return [inverse[0] * point_sums[0] + inverse[1] * point_sums[1] + inverse[2] * point_sums[2],
            inverse[1] * point_sums[0] + inverse[3] * point_sums[1] + inverse[4] * point_sums[2],
            inverse[2] * point_sums[0] + inverse[4] * point_sums[1] + inverse[5] * point_sums[2]]


def camera_rows(cam_jac, vector, weights):
    error_rows = []
    for row_index in range(2):
        running = cam_jac[9 * row_index].astype(jnp.float32) * vector[0][:, None]
        for column in range(1, 9):
            running = running + cam_jac[9 * row_index + column].astype(jnp.float32) * vector[column][:, None]
        error_rows.append(running * weights)
    return error_rows


def schur_apply(vector, cam_jac, point_jac, weights, owners, inverse, cam_damp):
    errors = camera_rows(cam_jac, vector, weights)
    point_sums = []
    for column in range(3):
        product = errors[0] * point_jac[column].astype(jnp.float32) + errors[1] * point_jac[3 + column].astype(jnp.float32)
        point_sums.append(jax.ops.segment_sum(product.reshape(-1), owners, num_segments=POINTS))
    values = apply_inverse(inverse, point_sums)
    picked = [member[owners].reshape(weights.shape) for member in values]
    adjusted = []
    for row_index in range(2):
        back_term = picked[0] * point_jac[3 * row_index].astype(jnp.float32)
        back_term = back_term + picked[1] * point_jac[3 * row_index + 1].astype(jnp.float32)
        back_term = back_term + picked[2] * point_jac[3 * row_index + 2].astype(jnp.float32)
        adjusted.append(errors[row_index] - weights * back_term)
    result = []
    for column in range(9):
        running = jnp.sum(cam_jac[column].astype(jnp.float32) * adjusted[0] + cam_jac[9 + column].astype(jnp.float32) * adjusted[1], axis=1)
        result.append(cam_damp * vector[column] + running)
    return jnp.stack(result)


def reference(cam_jac, point_jac, obs_point, obs_count, back_list, front_list, point_damp, cam_damp, right_side, start_guess):
    weights = slot_weights(obs_count, obs_point.shape[1])
    owners = global_points(obs_point, back_list, front_list)
    entries = []
    for lead_index, tail_index in ENTRY_PAIRS:
        product = point_jac[lead_index].astype(jnp.float32) * point_jac[tail_index].astype(jnp.float32)
        product = product + point_jac[3 + lead_index].astype(jnp.float32) * point_jac[3 + tail_index].astype(jnp.float32)
        running = jax.ops.segment_sum((product * weights).reshape(-1), owners, num_segments=POINTS)
        if lead_index == tail_index:
            running = running + point_damp
        entries.append(running)
    inverse = symmetric_inverse(entries)
    diagonal = []
    for column in range(9):
        first_sq = cam_jac[column].astype(jnp.float32) ** 2 + cam_jac[9 + column].astype(jnp.float32) ** 2
        diagonal.append(jnp.sum(first_sq * weights, axis=1) + cam_damp)
    precond = 1.0 / jnp.stack(diagonal)

    def operator(vector):
        return schur_apply(vector, cam_jac, point_jac, weights, owners, inverse, cam_damp)

    solution = start_guess
    residual = right_side - operator(solution)
    scaled = precond * residual
    direction = scaled
    inner_now = jnp.sum(residual * scaled)
    for iteration in range(ITERS):
        image = operator(direction)
        step_size = inner_now / jnp.sum(direction * image)
        solution = solution + step_size * direction
        residual = residual - step_size * image
        if iteration + 1 < ITERS:
            scaled = precond * residual
            inner_next = jnp.sum(residual * scaled)
            direction = scaled + (inner_next / inner_now) * direction
            inner_now = inner_next
    return solution, residual
```

```python
import functools

import jax
import jax.numpy as jnp
from jax import lax
from jax.experimental import pallas as pl
from jax.experimental.pallas import tpu as pltpu
from jax.sharding import PartitionSpec as P

ENTRY_PAIRS = ((0, 0), (0, 1), (0, 2), (1, 1), (1, 2), (2, 2))
F32, BF16, I32 = jnp.float32, jnp.bfloat16, jnp.int32
MESH = pl.DeviceIdType.MESH
LANES = 128
WIDE = 256
GROUP = 8
SPLITS = 3
FIRST_ROWS = (0, 9, 12)


def splits_of(value):
    terms = []
    for step in range(SPLITS):
        term = value.astype(BF16).astype(F32)
        terms.append(term)
        value = value - term
    return terms


def iota(shape, dim):
    return lax.broadcasted_iota(I32, shape, dim)


def dot_nt(left, right):
    return lax.dot_general(left, right, (((1,), (1,)), ((), ())), preferred_element_type=F32)


def symmetric_inverse(entries):
    cofactors = [
        entries[3] * entries[5] - entries[4] * entries[4],
        entries[2] * entries[4] - entries[1] * entries[5],
        entries[1] * entries[4] - entries[2] * entries[3],
        entries[0] * entries[5] - entries[2] * entries[2],
        entries[1] * entries[2] - entries[0] * entries[4],
        entries[0] * entries[3] - entries[1] * entries[1],
    ]
    determinant = entries[0] * cofactors[0] + entries[1] * cofactors[1] + entries[2] * cofactors[2]
    determinant = jnp.where(determinant > 0.0, determinant, 1.0)
    return [member / determinant for member in cofactors]


def apply_inverse(inverse, sums):
    return [
        inverse[0] * sums[0] + inverse[1] * sums[1] + inverse[2] * sums[2],
        inverse[1] * sums[0] + inverse[3] * sums[1] + inverse[4] * sums[2],
        inverse[2] * sums[0] + inverse[4] * sums[1] + inverse[5] * sums[2],
    ]


def kernel(
    n,
    cam_jac,
    point_jac,
    obs_point,
    obs_count,
    back_list,
    front_list,
    point_damp,
    cam_damp,
    right_side,
    start_guess,
    step_out,
    residual_out,
    lane_hot,
    spread,
    group_of,
    picked,
    to_next,
    to_prev,
    from_prev,
    from_next,
    dots_out,
    dots_in,
    next_send,
    next_recv,
    prev_send,
    prev_recv,
    dots_send,
    dots_recv,
):
    cams, slots = obs_point.shape
    points = point_damp.shape[1]
    border = back_list.shape[1]
    edge = border // LANES
    own_groups = points // WIDE
    me = lax.axis_index("seg")

    barrier = pltpu.get_barrier_semaphore()

    def greet(offset, carry):
        pl.semaphore_signal(
            barrier, inc=1, device_id=(lax.rem(me + offset, n),), device_id_type=MESH
        )
        return carry

    from_prev[...] = jnp.zeros_like(from_prev)
    from_next[...] = jnp.zeros_like(from_next)
    lax.fori_loop(1, n, greet, 0)

    listed = jnp.concatenate([back_list[...], front_list[...]], axis=1)
    total = 2 * border
    place = iota((1, total), 1)
    in_front = place >= border
    place = jnp.where(in_front, place - border, place)
    list_group = jnp.where(in_front, edge, 0) + lax.shift_right_logical(place, 7)
    list_lane = jnp.where(in_front, LANES, 0) + (place & (LANES - 1))
    row = iota((2 * own_groups, total), 0)
    code = jnp.where(row < own_groups, list_group + 1, list_lane)
    wanted = jnp.where(row < own_groups, row, row - own_groups)
    code = jnp.where(lax.shift_right_logical(listed, 8) == wanted, code, 0)
    hot = jnp.where(iota((WIDE, total), 0) == (listed & (WIDE - 1)), 1.0, 0.0).astype(BF16)
    table = dot_nt(code.astype(F32).astype(BF16), hot)
    table_group = table[:own_groups]
    table_lane = table[own_groups:]
    other = jnp.where(table_group == 0.0, 1.0, 0.0)
    before = jnp.where(iota((WIDE, WIDE), 0) < iota((WIDE, WIDE), 1), 1.0, 0.0).astype(BF16)
    rank = jnp.dot(other.astype(BF16), before, preferred_element_type=F32)
    counts = jnp.sum(other, axis=1, keepdims=True)
    table_row = iota((own_groups, WIDE), 0)
    for index in range(own_groups - 1):
        rank = rank + jnp.where(table_row > index, counts[index : index + 1], 0.0)
    rank = rank.astype(I32)
    is_other = other > 0.0
    table_group = jnp.where(
        is_other, (2 * edge + lax.shift_right_logical(rank, 8)).astype(F32), table_group - 1.0
    )
    table_lane = jnp.where(is_other, (rank & (WIDE - 1)).astype(F32), table_lane)
    table = jnp.concatenate([table_group, table_lane], axis=0).astype(BF16)

    eye = iota((cams, cams), 0) == iota((cams, cams), 1)

    def column(line):
        wide = jnp.broadcast_to(line, (cams, cams))
        return jnp.sum(jnp.where(eye, wide, jnp.zeros_like(wide)), axis=1, keepdims=True)

    def line(col):
        wide = jnp.broadcast_to(col, (cams, cams))
        return jnp.sum(jnp.where(eye, wide, 0.0), axis=0, keepdims=True)

    used_count = column(obs_count[...].astype(F32)).astype(I32)
    used = iota((cams, slots), 1) < used_count

    ids = obs_point[...]
    back_slot = ids - points
    front_slot = back_slot - border
    own = ids < points
    in_back = ids < points + border
    side_group = jnp.where(
        in_back, lax.shift_right_logical(back_slot, 7), edge + lax.shift_right_logical(front_slot, 7)
    )
    side_lane = jnp.where(
        in_back, LANES + (back_slot & (LANES - 1)), front_slot & (LANES - 1)
    )
    old_group = lax.shift_right_logical(ids, 8)
    old_lane = ids & (WIDE - 1)
    wide_row = iota((WIDE, slots), 0)
    look_row = iota((2 * own_groups, slots), 0)
    look_row = jnp.where(look_row < own_groups, look_row, look_row - own_groups)
    for cam in range(cams):
        pick = slice(cam, cam + 1)
        hot = jnp.where(wide_row == old_lane[pick], 1.0, 0.0).astype(BF16)
        found = jnp.dot(table, hot, preferred_element_type=F32)
        found = jnp.where(look_row == old_group[pick], found, 0.0)
        new_group = jnp.sum(found[:own_groups], axis=0, keepdims=True).astype(I32)
        new_lane = jnp.sum(found[own_groups:], axis=0, keepdims=True).astype(I32)
        new_group = jnp.where(own[pick], new_group, side_group[pick])
        new_lane = jnp.where(own[pick], new_lane, side_lane[pick])
        group_of[pick] = jnp.where(used[pick], new_group, -1)
        lane_hot[:, cam * slots : (cam + 1) * slots] = jnp.where(
            wide_row == new_lane, 1.0, 0.0
        ).astype(BF16)

    group_row = iota((GROUP, slots), 0)

    def point_sums(values):
        rows = len(values) * GROUP
        terms = [splits_of(value) for value in values]
        for cam in range(cams):
            mask = group_row == group_of[cam : cam + 1]
            blocks = [
                jnp.where(mask, terms[index][step][cam : cam + 1], 0.0)
                for step in range(SPLITS)
                for index in range(len(values))
            ]
            spread[: SPLITS * rows, cam * slots : (cam + 1) * slots] = jnp.concatenate(
                blocks, axis=0
            ).astype(BF16)
        sums = dot_nt(spread[: SPLITS * rows], lane_hot[...])
        whole = sums[(SPLITS - 1) * rows :]
        for step in reversed(range(SPLITS - 1)):
            whole = whole + sums[step * rows : (step + 1) * rows]
        return [whole[index * GROUP : (index + 1) * GROUP] for index in range(len(values))]

    def neighbour(where, turn, size):
        spot = FIRST_ROWS[turn]
        if where == "next":
            return pltpu.make_async_remote_copy(
                src_ref=to_next.at[pl.ds(spot, size)],
                dst_ref=from_prev.at[pl.ds(spot, size)],
                send_sem=next_send.at[turn],
                recv_sem=next_recv.at[turn],
                device_id=(lax.rem(me + 1, n),),
                device_id_type=MESH,
            )
        return pltpu.make_async_remote_copy(
            src_ref=to_prev.at[pl.ds(spot, size)],
            dst_ref=from_next.at[pl.ds(spot, size)],
            send_sem=prev_send.at[turn],
            recv_sem=prev_recv.at[turn],
            device_id=(lax.rem(me + n - 1, n),),
            device_id_type=MESH,
        )

    has_next = me < n - 1
    has_prev = me > 0

    def send(sums, turn):
        spot = FIRST_ROWS[turn]
        for index, member in enumerate(sums):
            to_next[spot + index] = member[:, :LANES]
            to_prev[spot + index] = member[:, LANES:]

        @pl.when(has_next)
        def _():
            neighbour("next", turn, len(sums)).start()

        @pl.when(has_prev)
        def _():
            neighbour("prev", turn, len(sums)).start()

    edge_row = iota((GROUP, LANES), 0) < 2 * edge

    def receive(sums, turn):
        spot = FIRST_ROWS[turn]
        @pl.when(has_next)
        def _():
            copy = neighbour("next", turn, len(sums))
            copy.wait_send()
            neighbour("prev", turn, len(sums)).wait_recv()

        @pl.when(has_prev)
        def _():
            copy = neighbour("prev", turn, len(sums))
            copy.wait_send()
            neighbour("next", turn, len(sums)).wait_recv()

        return [
            jnp.concatenate(
                [
                    member[:, :LANES] + jnp.where(edge_row, from_next[spot + index], 0.0),
                    member[:, LANES:] + jnp.where(edge_row, from_prev[spot + index], 0.0),
                ],
                axis=1,
            )
            for index, member in enumerate(sums)
        ]

    def jac(index):
        return cam_jac[index].astype(F32)

    def pjac(index):
        return point_jac[index].astype(F32)

    def errors_of(vector):
        rows = []
        for side in range(2):
            running = jac(9 * side) * vector[0]
            for entry in range(1, 9):
                running = running + jac(9 * side + entry) * vector[entry]
            rows.append(jnp.where(used, running, 0.0))
        return rows

    def products(errors):
        return [errors[0] * pjac(entry) + errors[1] * pjac(3 + entry) for entry in range(3)]

    def finish(vector, errors, sums):
        values = apply_inverse(inverse, sums)
        terms = [splits_of(value) for value in values]
        stacked = jnp.concatenate(
            [terms[index][step] for step in range(SPLITS) for index in range(3)], axis=0
        ).astype(BF16)
        rows = 3 * GROUP
        for cam in range(cams):
            found = jnp.dot(
                stacked,
                lane_hot[:, cam * slots : (cam + 1) * slots],
                preferred_element_type=F32,
            )
            whole = found[(SPLITS - 1) * rows :]
            for step in reversed(range(SPLITS - 1)):
                whole = whole + found[step * rows : (step + 1) * rows]
            mask = group_row == group_of[cam : cam + 1]
            for index in range(3):
                picked[index, cam : cam + 1] = jnp.sum(
                    jnp.where(mask, whole[index * GROUP : (index + 1) * GROUP], 0.0),
                    axis=0,
                    keepdims=True,
                )
        adjusted = []
        for side in range(2):
            back = picked[0] * pjac(3 * side)
            back = back + picked[1] * pjac(3 * side + 1)
            back = back + picked[2] * pjac(3 * side + 2)
            adjusted.append(errors[side] - back)
        return [
            damp * vector[entry]
            + jnp.sum(
                jac(entry) * adjusted[0] + jac(9 + entry) * adjusted[1], axis=1, keepdims=True
            )
            for entry in range(9)
        ]

    def dot_of(left, right):
        running = left[0] * right[0]
        for entry in range(1, 9):
            running = running + left[entry] * right[entry]
        return jnp.sum(running, axis=0, keepdims=True)

    dot_lane = iota((1, LANES), 1)

    def dots_copy(which, offset):
        return pltpu.make_async_remote_copy(
            src_ref=dots_out.at[which],
            dst_ref=dots_in.at[which, offset - 1],
            send_sem=dots_send.at[which],
            recv_sem=dots_recv.at[which],
            device_id=(lax.rem(me + offset, n),),
            device_id_type=MESH,
        )

    def send_dots(which, members):
        packed = jnp.zeros((1, LANES), F32)
        for index, member in enumerate(members):
            packed = jnp.where(dot_lane == index, member, packed)
        dots_out[which] = packed

        def one(offset, carry):
            dots_copy(which, offset).start()
            return carry

        lax.fori_loop(1, n, one, 0)
        return packed

    def receive_dots(which, packed, count):
        pltpu.make_async_copy(dots_in.at[which], dots_in.at[which], dots_recv.at[which]).wait()
        pltpu.make_async_copy(dots_in.at[which], dots_in.at[which], dots_send.at[which]).wait()
        whole = packed + jnp.sum(dots_in[which], axis=0)
        return [
            jnp.sum(jnp.where(dot_lane == index, whole, 0.0), axis=1, keepdims=True)
            for index in range(count)
        ]

    damp = column(cam_damp[...])
    start = [column(start_guess[entry : entry + 1]) for entry in range(9)]
    right = [column(right_side[entry : entry + 1]) for entry in range(9)]

    errors = errors_of(start)
    blocks = [
        pjac(lead) * pjac(tail) + pjac(3 + lead) * pjac(3 + tail) for lead, tail in ENTRY_PAIRS
    ]
    sums = point_sums(blocks + products(errors))

    damping = jnp.zeros((SPLITS * GROUP, WIDE), F32)
    damp_row = iota((GROUP, WIDE), 0)
    square_row = iota((WIDE, WIDE), 0)
    for index in range(own_groups):
        here = point_damp[:, index * WIDE : (index + 1) * WIDE]
        mask = damp_row == table_group[index : index + 1].astype(I32)
        block = jnp.concatenate([jnp.where(mask, term, 0.0) for term in splits_of(here)], axis=0)
        hot = jnp.where(
            square_row == table_lane[index : index + 1].astype(I32), 1.0, 0.0
        ).astype(BF16)
        damping = damping + dot_nt(block.astype(BF16), hot)
    moved = damping[(SPLITS - 1) * GROUP :]
    for step in reversed(range(SPLITS - 1)):
        moved = moved + damping[step * GROUP : (step + 1) * GROUP]
    for index, (lead, tail) in enumerate(ENTRY_PAIRS):
        if lead == tail:
            sums[index] = sums[index] + moved

    pl.semaphore_wait(barrier, n - 1)
    send(sums, 0)

    precond = []
    for entry in range(9):
        squared = jnp.where(used, jac(entry) ** 2 + jac(9 + entry) ** 2, 0.0)
        precond.append(1.0 / (jnp.sum(squared, axis=1, keepdims=True) + damp))

    sums = receive(sums, 0)
    inverse = symmetric_inverse(sums[:6])
    image = finish(start, errors, sums[6:])
    residual = [right[entry] - image[entry] for entry in range(9)]
    direction = [precond[entry] * residual[entry] for entry in range(9)]

    errors = errors_of(direction)
    sums = point_sums(products(errors))
    send(sums, 1)
    sums = receive(sums, 1)
    image = finish(direction, errors, sums)

    first = send_dots(0, [dot_of(residual, direction), dot_of(direction, image)])
    ahead = [precond[entry] * image[entry] for entry in range(9)]
    errors = errors_of(ahead)
    sums = point_sums(products(errors))
    send(sums, 2)
    sums = receive(sums, 2)
    further = finish(ahead, errors, sums)

    inner, curve = receive_dots(0, first, 2)
    step = inner / curve
    solution = [start[entry] + step * direction[entry] for entry in range(9)]
    residual = [residual[entry] - step * image[entry] for entry in range(9)]
    scaled = [precond[entry] * residual[entry] for entry in range(9)]
    applied = [image[entry] - step * further[entry] for entry in range(9)]
    second = send_dots(
        1,
        [
            dot_of(residual, scaled),
            dot_of(scaled, applied),
            dot_of(scaled, image) + dot_of(direction, applied),
        ],
    )
    inner_next, own_curve, cross = receive_dots(1, second, 3)
    ratio = inner_next / inner
    curve = own_curve + ratio * (cross + ratio * curve)
    step = inner_next / curve
    for entry in range(9):
        fresh = scaled[entry] + ratio * direction[entry]
        seen = applied[entry] + ratio * image[entry]
        step_out[entry : entry + 1] = line(solution[entry] + step * fresh)
        residual_out[entry : entry + 1] = line(residual[entry] - step * seen)


def solution(mesh):
    n = mesh.shape["seg"]

    def shards(
        cam_jac,
        point_jac,
        obs_point,
        obs_count,
        back_list,
        front_list,
        point_damp,
        cam_damp,
        right_side,
        start_guess,
    ):
        cams, slots = obs_point.shape
        observations = cams * slots
        vector = jax.ShapeDtypeStruct(right_side.shape, F32)
        return pl.pallas_call(
            functools.partial(kernel, n),
            out_shape=(vector, vector),
            in_specs=[pl.BlockSpec(memory_space=pltpu.VMEM)] * 10,
            out_specs=(pl.BlockSpec(memory_space=pltpu.VMEM),) * 2,
            scratch_shapes=[
                pltpu.VMEM((WIDE, observations), BF16),
                pltpu.VMEM((SPLITS * 9 * GROUP, observations), BF16),
                pltpu.VMEM((cams, slots), I32),
                pltpu.VMEM((3, cams, slots), F32),
                pltpu.VMEM((15, GROUP, LANES), F32),
                pltpu.VMEM((15, GROUP, LANES), F32),
                pltpu.VMEM((15, GROUP, LANES), F32),
                pltpu.VMEM((15, GROUP, LANES), F32),
                pltpu.VMEM((2, 1, LANES), F32),
                pltpu.VMEM((2, n - 1, 1, LANES), F32),
                pltpu.SemaphoreType.DMA((3,)),
                pltpu.SemaphoreType.DMA((3,)),
                pltpu.SemaphoreType.DMA((3,)),
                pltpu.SemaphoreType.DMA((3,)),
                pltpu.SemaphoreType.DMA((2,)),
                pltpu.SemaphoreType.DMA((2,)),
            ],
            compiler_params=pltpu.CompilerParams(
                collective_id=0, has_side_effects=True, vmem_limit_bytes=48 * 1024 * 1024
            ),
            name="schur_cg",
        )(
            cam_jac,
            point_jac,
            obs_point,
            obs_count.reshape(1, -1),
            back_list,
            front_list,
            point_damp.reshape(1, -1),
            cam_damp.reshape(1, -1),
            right_side,
            start_guess,
        )

    return jax.shard_map(
        shards,
        mesh=mesh,
        in_specs=(
            P(None, "seg", None),
            P(None, "seg", None),
            P("seg", None),
            P("seg"),
            P("seg", None),
            P("seg", None),
            P("seg"),
            P("seg"),
            P(None, "seg"),
            P(None, "seg"),
        ),
        out_specs=(P(None, "seg"), P(None, "seg")),
        check_vma=False,
    )
```

```python
import functools

import jax
import jax.numpy as jnp
from jax import lax
from jax.experimental import pallas as pl
from jax.experimental.pallas import tpu as pltpu
from jax.sharding import PartitionSpec as P

ENTRY_PAIRS = ((0, 0), (0, 1), (0, 2), (1, 1), (1, 2), (2, 2))
F32, BF16, I32 = jnp.float32, jnp.bfloat16, jnp.int32
MESH = pl.DeviceIdType.MESH
LANES = 128
WIDE = 256
GROUP = 8
SPLITS = 2
FIRST_ROWS = (0, 9, 12)
LOAD_ORDER = (
    "back_list",
    "front_list",
    "obs_count",
    "obs_point",
    "cam_damp",
    "start_guess",
    "right_side",
    "point_damp",
    "point_jac",
    "cam_jac",
)


def splits_of(value):
    terms = []
    for step in range(SPLITS):
        term = value.astype(BF16).astype(F32)
        terms.append(term)
        value = value - term
    return terms


def iota(shape, dim):
    return lax.broadcasted_iota(I32, shape, dim)


def dot_nt(left, right):
    return lax.dot_general(left, right, (((1,), (1,)), ((), ())), preferred_element_type=F32)


def symmetric_inverse(entries):
    cofactors = [
        entries[3] * entries[5] - entries[4] * entries[4],
        entries[2] * entries[4] - entries[1] * entries[5],
        entries[1] * entries[4] - entries[2] * entries[3],
        entries[0] * entries[5] - entries[2] * entries[2],
        entries[1] * entries[2] - entries[0] * entries[4],
        entries[0] * entries[3] - entries[1] * entries[1],
    ]
    determinant = entries[0] * cofactors[0] + entries[1] * cofactors[1] + entries[2] * cofactors[2]
    determinant = jnp.where(determinant > 0.0, determinant, 1.0)
    return [member / determinant for member in cofactors]


def apply_inverse(inverse, sums):
    return [
        inverse[0] * sums[0] + inverse[1] * sums[1] + inverse[2] * sums[2],
        inverse[1] * sums[0] + inverse[3] * sums[1] + inverse[4] * sums[2],
        inverse[2] * sums[0] + inverse[4] * sums[1] + inverse[5] * sums[2],
    ]


def kernel(
    n,
    cam_jac_hbm,
    point_jac_hbm,
    obs_point_hbm,
    obs_count_hbm,
    back_list_hbm,
    front_list_hbm,
    point_damp_hbm,
    cam_damp_hbm,
    right_side_hbm,
    start_guess_hbm,
    step_out,
    residual_out,
    lane_hot,
    spread,
    group_of,
    picked,
    to_next,
    to_prev,
    from_prev,
    from_next,
    dots_out,
    dots_in,
    next_send,
    next_recv,
    prev_send,
    prev_recv,
    dots_send,
    dots_recv,
    cam_jac,
    point_jac,
    obs_point,
    obs_count,
    back_list,
    front_list,
    point_damp,
    cam_damp,
    right_side,
    start_guess,
    load_sem,
):
    cams, slots = obs_point.shape
    points = point_damp.shape[1]
    border = back_list.shape[1]
    edge = border // LANES
    own_groups = points // WIDE
    me = lax.axis_index("seg")

    loads = {
        "cam_jac": pltpu.make_async_copy(cam_jac_hbm, cam_jac, load_sem.at[0]),
        "point_jac": pltpu.make_async_copy(point_jac_hbm, point_jac, load_sem.at[1]),
        "obs_point": pltpu.make_async_copy(obs_point_hbm, obs_point, load_sem.at[2]),
        "obs_count": pltpu.make_async_copy(obs_count_hbm, obs_count, load_sem.at[3]),
        "back_list": pltpu.make_async_copy(back_list_hbm, back_list, load_sem.at[4]),
        "front_list": pltpu.make_async_copy(front_list_hbm, front_list, load_sem.at[5]),
        "point_damp": pltpu.make_async_copy(point_damp_hbm, point_damp, load_sem.at[6]),
        "cam_damp": pltpu.make_async_copy(cam_damp_hbm, cam_damp, load_sem.at[7]),
        "right_side": pltpu.make_async_copy(right_side_hbm, right_side, load_sem.at[8]),
        "start_guess": pltpu.make_async_copy(start_guess_hbm, start_guess, load_sem.at[9]),
    }
    for name in LOAD_ORDER:
        loads[name].start()

    barrier = pltpu.get_barrier_semaphore()

    def greet(offset, carry):
        pl.semaphore_signal(
            barrier, inc=1, device_id=(lax.rem(me + offset, n),), device_id_type=MESH
        )
        return carry

    from_prev[...] = jnp.zeros_like(from_prev)
    from_next[...] = jnp.zeros_like(from_next)
    lax.fori_loop(1, n, greet, 0)

    loads["back_list"].wait()
    loads["front_list"].wait()
    listed = jnp.concatenate([back_list[...], front_list[...]], axis=1)
    total = 2 * border
    place = iota((1, total), 1)
    in_front = place >= border
    place = jnp.where(in_front, place - border, place)
    list_group = jnp.where(in_front, edge, 0) + lax.shift_right_logical(place, 7)
    list_lane = jnp.where(in_front, LANES, 0) + (place & (LANES - 1))
    row = iota((2 * own_groups, total), 0)
    code = jnp.where(row < own_groups, list_group + 1, list_lane)
    wanted = jnp.where(row < own_groups, row, row - own_groups)
    code = jnp.where(lax.shift_right_logical(listed, 8) == wanted, code, 0)
    hot = jnp.where(iota((WIDE, total), 0) == (listed & (WIDE - 1)), 1.0, 0.0).astype(BF16)
    table = dot_nt(code.astype(F32).astype(BF16), hot)
    table_group = table[:own_groups]
    table_lane = table[own_groups:]
    other = jnp.where(table_group == 0.0, 1.0, 0.0)
    before = jnp.where(iota((WIDE, WIDE), 0) < iota((WIDE, WIDE), 1), 1.0, 0.0).astype(BF16)
    rank = jnp.dot(other.astype(BF16), before, preferred_element_type=F32)
    counts = jnp.sum(other, axis=1, keepdims=True)
    table_row = iota((own_groups, WIDE), 0)
    for index in range(own_groups - 1):
        rank = rank + jnp.where(table_row > index, counts[index : index + 1], 0.0)
    rank = rank.astype(I32)
    is_other = other > 0.0
    table_group = jnp.where(
        is_other, (2 * edge + lax.shift_right_logical(rank, 8)).astype(F32), table_group - 1.0
    )
    table_lane = jnp.where(is_other, (rank & (WIDE - 1)).astype(F32), table_lane)
    table = jnp.concatenate([table_group, table_lane], axis=0).astype(BF16)

    eye = iota((cams, cams), 0) == iota((cams, cams), 1)

    def column(line):
        wide = jnp.broadcast_to(line, (cams, cams))
        return jnp.sum(jnp.where(eye, wide, jnp.zeros_like(wide)), axis=1, keepdims=True)

    def line(col):
        wide = jnp.broadcast_to(col, (cams, cams))
        return jnp.sum(jnp.where(eye, wide, 0.0), axis=0, keepdims=True)

    loads["obs_count"].wait()
    loads["obs_point"].wait()
    used_count = column(obs_count[...].astype(F32)).astype(I32)
    used = iota((cams, slots), 1) < used_count

    ids = obs_point[...]
    back_slot = ids - points
    front_slot = back_slot - border
    own = ids < points
    in_back = ids < points + border
    side_group = jnp.where(
        in_back, lax.shift_right_logical(back_slot, 7), edge + lax.shift_right_logical(front_slot, 7)
    )
    side_lane = jnp.where(
        in_back, LANES + (back_slot & (LANES - 1)), front_slot & (LANES - 1)
    )
    old_group = lax.shift_right_logical(ids, 8)
    old_lane = ids & (WIDE - 1)
    wide_row = iota((WIDE, slots), 0)
    look_row = iota((2 * own_groups, slots), 0)
    look_row = jnp.where(look_row < own_groups, look_row, look_row - own_groups)
    for cam in range(cams):
        pick = slice(cam, cam + 1)
        hot = jnp.where(wide_row == old_lane[pick], 1.0, 0.0).astype(BF16)
        found = jnp.dot(table, hot, preferred_element_type=F32)
        found = jnp.where(look_row == old_group[pick], found, 0.0)
        new_group = jnp.sum(found[:own_groups], axis=0, keepdims=True).astype(I32)
        new_lane = jnp.sum(found[own_groups:], axis=0, keepdims=True).astype(I32)
        new_group = jnp.where(own[pick], new_group, side_group[pick])
        new_lane = jnp.where(own[pick], new_lane, side_lane[pick])
        group_of[pick] = jnp.where(used[pick], new_group, -1)
        lane_hot[:, cam * slots : (cam + 1) * slots] = jnp.where(
            wide_row == new_lane, 1.0, 0.0
        ).astype(BF16)

    group_row = iota((GROUP, slots), 0)

    def point_sums(values):
        rows = len(values) * GROUP
        terms = [splits_of(value) for value in values]
        for cam in range(cams):
            mask = group_row == group_of[cam : cam + 1]
            blocks = [
                jnp.where(mask, terms[index][step][cam : cam + 1], 0.0)
                for step in range(SPLITS)
                for index in range(len(values))
            ]
            spread[: SPLITS * rows, cam * slots : (cam + 1) * slots] = jnp.concatenate(
                blocks, axis=0
            ).astype(BF16)
        sums = dot_nt(spread[: SPLITS * rows], lane_hot[...])
        whole = sums[(SPLITS - 1) * rows :]
        for step in reversed(range(SPLITS - 1)):
            whole = whole + sums[step * rows : (step + 1) * rows]
        return [whole[index * GROUP : (index + 1) * GROUP] for index in range(len(values))]

    def neighbour(where, turn, size):
        spot = FIRST_ROWS[turn]
        if where == "next":
            return pltpu.make_async_remote_copy(
                src_ref=to_next.at[pl.ds(spot, size)],
                dst_ref=from_prev.at[pl.ds(spot, size)],
                send_sem=next_send.at[turn],
                recv_sem=next_recv.at[turn],
                device_id=(lax.rem(me + 1, n),),
                device_id_type=MESH,
            )
        return pltpu.make_async_remote_copy(
            src_ref=to_prev.at[pl.ds(spot, size)],
            dst_ref=from_next.at[pl.ds(spot, size)],
            send_sem=prev_send.at[turn],
            recv_sem=prev_recv.at[turn],
            device_id=(lax.rem(me + n - 1, n),),
            device_id_type=MESH,
        )

    has_next = me < n - 1
    has_prev = me > 0

    def send(sums, turn):
        spot = FIRST_ROWS[turn]
        for index, member in enumerate(sums):
            to_next[spot + index] = member[:, :LANES]
            to_prev[spot + index] = member[:, LANES:]

        @pl.when(has_next)
        def _():
            neighbour("next", turn, len(sums)).start()

        @pl.when(has_prev)
        def _():
            neighbour("prev", turn, len(sums)).start()

    edge_row = iota((GROUP, LANES), 0) < 2 * edge

    def receive(sums, turn):
        spot = FIRST_ROWS[turn]
        @pl.when(has_next)
        def _():
            copy = neighbour("next", turn, len(sums))
            copy.wait_send()
            neighbour("prev", turn, len(sums)).wait_recv()

        @pl.when(has_prev)
        def _():
            copy = neighbour("prev", turn, len(sums))
            copy.wait_send()
            neighbour("next", turn, len(sums)).wait_recv()

        return [
            jnp.concatenate(
                [
                    member[:, :LANES] + jnp.where(edge_row, from_next[spot + index], 0.0),
                    member[:, LANES:] + jnp.where(edge_row, from_prev[spot + index], 0.0),
                ],
                axis=1,
            )
            for index, member in enumerate(sums)
        ]

    def jac(index):
        return cam_jac[index].astype(F32)

    def pjac(index):
        return point_jac[index].astype(F32)

    def errors_of(vector):
        rows = []
        for side in range(2):
            running = jac(9 * side) * vector[0]
            for entry in range(1, 9):
                running = running + jac(9 * side + entry) * vector[entry]
            rows.append(jnp.where(used, running, 0.0))
        return rows

    def products(errors):
        return [errors[0] * pjac(entry) + errors[1] * pjac(3 + entry) for entry in range(3)]

    def finish(vector, errors, values):
        terms = [splits_of(value) for value in values]
        stacked = jnp.concatenate(
            [terms[index][step] for step in range(SPLITS) for index in range(3)], axis=0
        ).astype(BF16)
        rows = 3 * GROUP
        for cam in range(cams):
            found = jnp.dot(
                stacked,
                lane_hot[:, cam * slots : (cam + 1) * slots],
                preferred_element_type=F32,
            )
            whole = found[(SPLITS - 1) * rows :]
            for step in reversed(range(SPLITS - 1)):
                whole = whole + found[step * rows : (step + 1) * rows]
            mask = group_row == group_of[cam : cam + 1]
            for index in range(3):
                picked[index, cam : cam + 1] = jnp.sum(
                    jnp.where(mask, whole[index * GROUP : (index + 1) * GROUP], 0.0),
                    axis=0,
                    keepdims=True,
                )
        adjusted = []
        for side in range(2):
            back = picked[0] * pjac(3 * side)
            back = back + picked[1] * pjac(3 * side + 1)
            back = back + picked[2] * pjac(3 * side + 2)
            adjusted.append(errors[side] - back)
        return [
            damp * vector[entry]
            + jnp.sum(
                jac(entry) * adjusted[0] + jac(9 + entry) * adjusted[1], axis=1, keepdims=True
            )
            for entry in range(9)
        ]

    def dot_of(left, right):
        running = left[0] * right[0]
        for entry in range(1, 9):
            running = running + left[entry] * right[entry]
        return jnp.sum(running, axis=0, keepdims=True)

    dot_lane = iota((1, LANES), 1)

    def dots_copy(which, offset):
        return pltpu.make_async_remote_copy(
            src_ref=dots_out.at[which],
            dst_ref=dots_in.at[which, offset - 1],
            send_sem=dots_send.at[which],
            recv_sem=dots_recv.at[which],
            device_id=(lax.rem(me + offset, n),),
            device_id_type=MESH,
        )

    def send_dots(which, members):
        packed = jnp.zeros((1, LANES), F32)
        for index, member in enumerate(members):
            packed = jnp.where(dot_lane == index, member, packed)
        dots_out[which] = packed

        def one(offset, carry):
            dots_copy(which, offset).start()
            return carry

        lax.fori_loop(1, n, one, 0)
        return packed

    def receive_dots(which, packed, count):
        pltpu.make_async_copy(dots_in.at[which], dots_in.at[which], dots_recv.at[which]).wait()
        pltpu.make_async_copy(dots_in.at[which], dots_in.at[which], dots_send.at[which]).wait()
        whole = packed + jnp.sum(dots_in[which], axis=0)
        return [
            jnp.sum(jnp.where(dot_lane == index, whole, 0.0), axis=1, keepdims=True)
            for index in range(count)
        ]

    for name in LOAD_ORDER[4:]:
        loads[name].wait()
    damp = column(cam_damp[...])
    start = [column(start_guess[entry : entry + 1]) for entry in range(9)]
    right = [column(right_side[entry : entry + 1]) for entry in range(9)]

    errors = errors_of(start)
    blocks = [
        pjac(lead) * pjac(tail) + pjac(3 + lead) * pjac(3 + tail) for lead, tail in ENTRY_PAIRS
    ]
    sums = point_sums(blocks + products(errors))

    damping = jnp.zeros((SPLITS * GROUP, WIDE), F32)
    damp_row = iota((GROUP, WIDE), 0)
    square_row = iota((WIDE, WIDE), 0)
    for index in range(own_groups):
        here = point_damp[:, index * WIDE : (index + 1) * WIDE]
        mask = damp_row == table_group[index : index + 1].astype(I32)
        block = jnp.concatenate([jnp.where(mask, term, 0.0) for term in splits_of(here)], axis=0)
        hot = jnp.where(
            square_row == table_lane[index : index + 1].astype(I32), 1.0, 0.0
        ).astype(BF16)
        damping = damping + dot_nt(block.astype(BF16), hot)
    moved = damping[(SPLITS - 1) * GROUP :]
    for step in reversed(range(SPLITS - 1)):
        moved = moved + damping[step * GROUP : (step + 1) * GROUP]
    for index, (lead, tail) in enumerate(ENTRY_PAIRS):
        if lead == tail:
            sums[index] = sums[index] + moved

    pl.semaphore_wait(barrier, n - 1)
    send(sums, 0)

    precond = []
    for entry in range(9):
        squared = jnp.where(used, jac(entry) ** 2 + jac(9 + entry) ** 2, 0.0)
        precond.append(1.0 / (jnp.sum(squared, axis=1, keepdims=True) + damp))

    sums = receive(sums, 0)
    inverse = symmetric_inverse(sums[:6])
    image = finish(start, errors, apply_inverse(inverse, sums[6:]))
    residual = [right[entry] - image[entry] for entry in range(9)]
    direction = [precond[entry] * residual[entry] for entry in range(9)]

    errors = errors_of(direction)
    sums = point_sums(products(errors))
    send(sums, 1)
    sums = receive(sums, 1)
    values = apply_inverse(inverse, sums)
    image = finish(direction, errors, values)

    first = send_dots(0, [dot_of(residual, direction), dot_of(direction, image)])
    ahead = [precond[entry] * image[entry] for entry in range(9)]
    errors_ahead = errors_of(ahead)
    sums_ahead = point_sums(products(errors_ahead))
    send(sums_ahead, 2)
    sums_ahead = receive(sums_ahead, 2)
    values_ahead = apply_inverse(inverse, sums_ahead)

    inner, curve = receive_dots(0, first, 2)
    step = inner / curve
    solution = [start[entry] + step * direction[entry] for entry in range(9)]
    residual = [residual[entry] - step * image[entry] for entry in range(9)]
    scaled = [precond[entry] * residual[entry] for entry in range(9)]

    quadratic = jnp.zeros((cams, 1), F32)
    for entry in range(9):
        quadratic = quadratic + damp * scaled[entry] * scaled[entry]
    squares = (errors[0] - step * errors_ahead[0]) ** 2 + (errors[1] - step * errors_ahead[1]) ** 2
    quadratic = quadratic + jnp.sum(squares, axis=1, keepdims=True)
    quadratic = jnp.sum(quadratic, axis=0, keepdims=True)
    point_part = jnp.zeros((GROUP, WIDE), F32)
    for index in range(3):
        point_part = point_part + (sums[index] - step * sums_ahead[index]) * (
            values[index] - step * values_ahead[index]
        )
    part_row = iota((GROUP, WIDE), 0)
    part_left = iota((GROUP, WIDE), 1) < LANES
    own_row = jnp.where(part_left, part_row, part_row - edge)
    is_own = jnp.where(part_left, edge - 1 - own_row, own_row) >= 0
    is_own = is_own | (part_row >= 2 * edge)
    point_part = jnp.sum(jnp.where(is_own, point_part, 0.0), axis=1, keepdims=True)
    quadratic = quadratic - jnp.sum(point_part, axis=0, keepdims=True)
    second = send_dots(1, [dot_of(residual, scaled), quadratic, dot_of(scaled, image)])

    further = finish(ahead, errors_ahead, values_ahead)
    applied = [image[entry] - step * further[entry] for entry in range(9)]
    inner_next, own_curve, cross = receive_dots(1, second, 3)
    ratio = inner_next / inner
    curve = own_curve + ratio * (2.0 * cross + ratio * curve)
    step = inner_next / curve
    for entry in range(9):
        fresh = scaled[entry] + ratio * direction[entry]
        seen = applied[entry] + ratio * image[entry]
        step_out[entry : entry + 1] = line(solution[entry] + step * fresh)
        residual_out[entry : entry + 1] = line(residual[entry] - step * seen)


def solution(mesh):
    n = mesh.shape["seg"]

    def shards(
        cam_jac,
        point_jac,
        obs_point,
        obs_count,
        back_list,
        front_list,
        point_damp,
        cam_damp,
        right_side,
        start_guess,
    ):
        cams, slots = obs_point.shape
        observations = cams * slots
        operands = (
            cam_jac,
            point_jac,
            obs_point,
            obs_count.reshape(1, -1),
            back_list,
            front_list,
            point_damp.reshape(1, -1),
            cam_damp.reshape(1, -1),
            right_side,
            start_guess,
        )
        vector = jax.ShapeDtypeStruct(right_side.shape, F32)
        return pl.pallas_call(
            functools.partial(kernel, n),
            out_shape=(vector, vector),
            in_specs=[pl.BlockSpec(memory_space=pltpu.HBM)] * 10,
            out_specs=(pl.BlockSpec(memory_space=pltpu.VMEM),) * 2,
            scratch_shapes=[
                pltpu.VMEM((WIDE, observations), BF16),
                pltpu.VMEM((SPLITS * 9 * GROUP, observations), BF16),
                pltpu.VMEM((cams, slots), I32),
                pltpu.VMEM((3, cams, slots), F32),
                pltpu.VMEM((15, GROUP, LANES), F32),
                pltpu.VMEM((15, GROUP, LANES), F32),
                pltpu.VMEM((15, GROUP, LANES), F32),
                pltpu.VMEM((15, GROUP, LANES), F32),
                pltpu.VMEM((2, 1, LANES), F32),
                pltpu.VMEM((2, n - 1, 1, LANES), F32),
                pltpu.SemaphoreType.DMA((3,)),
                pltpu.SemaphoreType.DMA((3,)),
                pltpu.SemaphoreType.DMA((3,)),
                pltpu.SemaphoreType.DMA((3,)),
                pltpu.SemaphoreType.DMA((2,)),
                pltpu.SemaphoreType.DMA((2,)),
                *[pltpu.VMEM(member.shape, member.dtype) for member in operands],
                pltpu.SemaphoreType.DMA((len(operands),)),
            ],
            compiler_params=pltpu.CompilerParams(
                collective_id=0, has_side_effects=True, vmem_limit_bytes=56 * 1024 * 1024
            ),
            name="schur_cg",
        )(*operands)

    return jax.shard_map(
        shards,
        mesh=mesh,
        in_specs=(
            P(None, "seg", None),
            P(None, "seg", None),
            P("seg", None),
            P("seg"),
            P("seg", None),
            P("seg", None),
            P("seg"),
            P("seg"),
            P(None, "seg"),
            P(None, "seg"),
        ),
        out_specs=(P(None, "seg"), P(None, "seg")),
        check_vma=False,
    )
```
